32 devices in a mesh: dp: 1 (over z), tp: 32 (over y, x, core).
Axes of the slice: x: 4, y: 4, z: 1, core: 2. Of those that a mesh axis runs over, the one named last changes fastest.
The devices are a block of a 4x4x8 slice.
Arguments:
- tokens_in: bfloat16 [32, 256, 4096], P('dp')
- ln_gain: float32 [4096], replicated
- ln_bias: float32 [4096], replicated
- w_qkv: bfloat16 [4096, 32, 384], P(None, 'tp')
- w_out: bfloat16 [4096, 4096], P('tp')
- w_up: bfloat16 [4096, 16384], P(None, 'tp')
- w_down: bfloat16 [16384, 4096], P('tp')
- grad_out: bfloat16 [32, 256, 4096], P('dp')
Outputs:
- output 1: bfloat16 [32, 256, 4096], P('dp')
- output 2: bfloat16 [4096, 32, 384], P('dp', 'tp')
- output 3: bfloat16 [4096, 4096], P(('dp', 'tp'))
- output 4: bfloat16 [4096, 16384], P('dp', 'tp')
- output 5: bfloat16 [16384, 4096], P(('dp', 'tp'))
All inputs are finite; a program needn't handle non-finite values.
Results may differ from the reference program's by a relative error of at most 0.0114769.
Values are sent between devices in bfloat16 or wider.
A program may use at most 768 MiB of HBM per device.

```python
import jax
import jax.numpy as jnp
from jax import lax

GROUP_ROWS = 32
SEQ_LEN = 256
DMODEL = 4096
FFN_DIM = 16384
Q_HEADS = 32
KV_HEADS = 32
HEAD_DIM = 128

LN_EPS = 1e-5
GELU_COEF = 0.7071067811865476
PDF_COEF = 0.3989422804014327
Q_PER_GROUP = Q_HEADS // KV_HEADS
GROUP_COLS = (Q_PER_GROUP + 2) * HEAD_DIM


def setup_inputs(seed: int = 0, part: int = 0) -> dict:
    shared_keys = jax.random.split(jax.random.key(seed), 6)
    part_keys = jax.random.split(jax.random.fold_in(jax.random.key(seed + 1), part), 2)
    act_shape = (GROUP_ROWS, SEQ_LEN, DMODEL)
    tokens_in = jax.random.normal(part_keys[0], act_shape, jnp.float32).astype(jnp.bfloat16)
    grad_out = jax.random.normal(part_keys[1], act_shape, jnp.float32).astype(jnp.bfloat16)
    ln_gain = 1.0 + 0.3 * jax.random.normal(shared_keys[0], (DMODEL,), jnp.float32)
    ln_bias = 0.3 * jax.random.normal(shared_keys[1], (DMODEL,), jnp.float32)
    w_qkv = (jax.random.normal(shared_keys[2], (DMODEL, KV_HEADS, GROUP_COLS), jnp.float32) * DMODEL ** -0.5).astype(jnp.bfloat16)
    w_out = (jax.random.normal(shared_keys[3], (Q_HEADS * HEAD_DIM, DMODEL), jnp.float32) * (Q_HEADS * HEAD_DIM) ** -0.5).astype(jnp.bfloat16)
    w_up = (jax.random.normal(shared_keys[4], (DMODEL, FFN_DIM), jnp.float32) * DMODEL ** -0.5).astype(jnp.bfloat16)
    w_down = (jax.random.normal(shared_keys[5], (FFN_DIM, DMODEL), jnp.float32) * FFN_DIM ** -0.5).astype(jnp.bfloat16)
    return dict(tokens_in=tokens_in, ln_gain=ln_gain, ln_bias=ln_bias, w_qkv=w_qkv, w_out=w_out, w_up=w_up, w_down=w_down, grad_out=grad_out)


def attend_row(row_pair):
    qkv_row, dout_row = row_pair
    q_row = qkv_row[:, :, :Q_PER_GROUP].astype(jnp.float32)
    k_row = qkv_row[:, :, Q_PER_GROUP].astype(jnp.float32)
    v_row = qkv_row[:, :, Q_PER_GROUP + 1].astype(jnp.float32)
    dout_f32 = dout_row.astype(jnp.float32)
    score_scale = HEAD_DIM ** -0.5
    causal = jnp.arange(SEQ_LEN)[:, None] >= jnp.arange(SEQ_LEN)[None, :]
    scores = jnp.einsum('qgpd,kgd->gpqk', q_row, k_row) * score_scale
    soft_probs = jax.nn.softmax(jnp.where(causal, scores, -1e30), axis=-1)
    probs_bf = soft_probs.astype(jnp.bfloat16).astype(jnp.float32)
    attn_out = jnp.einsum('gpqk,kgd->qgpd', probs_bf, v_row).astype(jnp.bfloat16)
    d_probs = jnp.einsum('qgpd,kgd->gpqk', dout_f32, v_row)
    d_val = jnp.einsum('gpqk,qgpd->kgd', probs_bf, dout_f32)
    row_dot = jnp.sum(soft_probs * d_probs, axis=-1, keepdims=True)
    d_scores = (soft_probs * (d_probs - row_dot) * score_scale).astype(jnp.bfloat16).astype(jnp.float32)
    d_query = jnp.einsum('gpqk,kgd->qgpd', d_scores, k_row)
    d_key = jnp.einsum('gpqk,qgpd->kgd', d_scores, q_row)
    d_qkv = jnp.concatenate([d_query, d_key[:, :, None], d_val[:, :, None]], axis=2)
    return attn_out, d_qkv.astype(jnp.bfloat16)


def reference(tokens_in, ln_gain, ln_bias, w_qkv, w_out, w_up, w_down, grad_out):
    tok_count = GROUP_ROWS * SEQ_LEN
    x_flat = tokens_in.reshape(tok_count, DMODEL).astype(jnp.float32)
    dy_flat = grad_out.reshape(tok_count, DMODEL)
    centered = x_flat - jnp.mean(x_flat, axis=-1, keepdims=True)
    inv_std = lax.rsqrt(jnp.mean(centered * centered, axis=-1, keepdims=True) + LN_EPS)
    x_hat = centered * inv_std
    normed = (x_hat * ln_gain + ln_bias).astype(jnp.bfloat16)
    w_qkv_flat = w_qkv.reshape(DMODEL, KV_HEADS * GROUP_COLS)
    qkv_proj = jnp.dot(normed, w_qkv_flat, preferred_element_type=jnp.float32).astype(jnp.bfloat16)
    d_attn = jnp.dot(dy_flat, w_out.T, preferred_element_type=jnp.float32).astype(jnp.bfloat16)
    attn_out, d_qkv = lax.map(attend_row, (qkv_proj.reshape(GROUP_ROWS, SEQ_LEN, KV_HEADS, Q_PER_GROUP + 2, HEAD_DIM), d_attn.reshape(GROUP_ROWS, SEQ_LEN, KV_HEADS, Q_PER_GROUP, HEAD_DIM)))
    attn_flat = attn_out.reshape(tok_count, Q_HEADS * HEAD_DIM)
    d_qkv_flat = d_qkv.reshape(tok_count, KV_HEADS * GROUP_COLS)
    hidden = jnp.dot(normed, w_up, preferred_element_type=jnp.float32)
    gauss_cdf = 0.5 * (1.0 + lax.erf(hidden * GELU_COEF))
    gelu_out = (hidden * gauss_cdf).astype(jnp.bfloat16)
    d_act = jnp.dot(dy_flat, w_down.T, preferred_element_type=jnp.float32)
    d_hidden = (d_act * (gauss_cdf + hidden * PDF_COEF * jnp.exp(-0.5 * hidden * hidden))).astype(jnp.bfloat16)
    grad_qkv = jnp.dot(normed.T, d_qkv_flat, preferred_element_type=jnp.float32).astype(jnp.bfloat16).reshape(DMODEL, KV_HEADS, GROUP_COLS)
    grad_wout = jnp.dot(attn_flat.T, dy_flat, preferred_element_type=jnp.float32).astype(jnp.bfloat16)
    grad_up = jnp.dot(normed.T, d_hidden, preferred_element_type=jnp.float32).astype(jnp.bfloat16)
    grad_down = jnp.dot(gelu_out.T, dy_flat, preferred_element_type=jnp.float32).astype(jnp.bfloat16)
    d_norm = jnp.dot(d_qkv_flat, w_qkv_flat.T, preferred_element_type=jnp.float32) + jnp.dot(d_hidden, w_up.T, preferred_element_type=jnp.float32)
    d_hat = d_norm * ln_gain
    grad_x = inv_std * (d_hat - jnp.mean(d_hat, axis=-1, keepdims=True) - x_hat * jnp.mean(d_hat * x_hat, axis=-1, keepdims=True))
    grad_in = (dy_flat.astype(jnp.float32) + grad_x).astype(jnp.bfloat16).reshape(GROUP_ROWS, SEQ_LEN, DMODEL)
    return (grad_in, grad_qkv, grad_wout, grad_up, grad_down)
```

```python
import functools
import jax
import jax.numpy as jnp
from jax import lax
from jax.experimental import pallas as pl
from jax.experimental.pallas import tpu as pltpu
from jax.sharding import PartitionSpec as P

EPS = 1e-5
GELU_COEF = 0.7071067811865476
PDF_COEF = 0.3989422804014327
F32 = jnp.float32
BF = jnp.bfloat16
VMEM_LIMIT = 64 * 2**20 - 65536
CORES = 2
COLORS = 4


def dg(a, b, ca, cb):
    return lax.dot_general(a, b, (((ca,), (cb,)), ((), ())), preferred_element_type=F32)


def normalize(x):
    x = x.astype(F32)
    c = x - jnp.mean(x, axis=-1, keepdims=True)
    r = lax.rsqrt(jnp.mean(c * c, axis=-1, keepdims=True) + EPS)
    return c * r, r


def attend(q, k, v, do, scale):
    S = q.shape[1]
    st = dg(k, q, 0, 0) * scale
    ki = lax.broadcasted_iota(jnp.int32, (S, S), 0)
    qi = lax.broadcasted_iota(jnp.int32, (S, S), 1)
    st = jnp.where(ki <= qi, st, -1e30)
    e = jnp.exp(st - jnp.max(st, axis=0, keepdims=True))
    p = e / jnp.sum(e, axis=0, keepdims=True)
    pb = p.astype(BF)
    o = dg(v, pb, 1, 0)
    dp = dg(v, do, 0, 0)
    dv = dg(do, pb, 1, 1)
    rd = jnp.sum(p * dp, axis=0, keepdims=True)
    ds = (p * (dp - rd) * scale).astype(BF)
    dq = dg(k, ds, 1, 0)
    dk = dg(q, ds, 1, 1)
    return o.astype(BF), dq.astype(BF), dk.astype(BF), dv.astype(BF)


class Place:
    def __init__(self, axis, side):
        self.axis, self.side = axis, side
        i = lax.axis_index(axis)
        self.c = lax.rem(i, CORES)
        chip = lax.div(i, CORES)
        self.x = lax.rem(chip, side)
        self.y = lax.div(chip, side)

    def index(self, x, y, c):
        return (y * self.side + x) * CORES + c

    def step(self, along, by):
        n = self.side
        if along == "x":
            return self.index(lax.rem(self.x + by + n, n), self.y, self.c)
        return self.index(self.x, lax.rem(self.y + by + n, n), self.c)

    def peer(self):
        return self.index(self.x, self.y, 1 - self.c)

    def block(self, along, by):
        n = self.side
        return lax.rem((self.x if along == "x" else self.y) + by + 2 * n, n)

    def partners(self):
        return [self.step("x", 1), self.step("x", -1), self.step("y", 1), self.step("y", -1), self.peer()]

    def greet(self):
        sem = pltpu.get_barrier_semaphore()
        who = self.partners()
        for w in who:
            pl.semaphore_signal(sem, inc=1, device_id={self.axis: w}, device_id_type=pl.DeviceIdType.MESH)
        pl.semaphore_wait(sem, len(who))


RINGS = (("x", "y", 1), ("x", "y", -1), ("y", "x", 1), ("y", "x", -1))


def forward_kernel(axis, side, S, d, C, F, nt, NB,
                   x0_ref, x_ref, dy_ref, g_ref, b_ref, wt_ref, wd_ref, xh_ref, dyh_ref,
                   lnh_ref, dc_ref, og_ref, sh_ref,
                   ln_s, h_s, da_s, qkv_s, do_s, dct_s, p_s, q_s, r1_s, r2_s, fx_s, fd_s, fo_s,
                   ln_sem, s0_send, s0_recv, s1_send, s1_recv, s2_send, s2_recv, f_sem, fo_sem):
    TM, D = x_ref.shape
    n = side
    me = Place(axis, side)
    g = pl.program_id(0)
    slot = lax.rem(g, 2)
    nxt = 1 - slot
    nu = nt // 2
    CW = D // COLORS
    QB = q_s.shape[0]
    RB = r1_s.shape[0]
    RR = q_s.shape[3]

    def copy_to(src, dst, ssem, rsem, dev):
        return pltpu.make_async_remote_copy(src_ref=src, dst_ref=dst, send_sem=ssem, recv_sem=rsem,
                                            device_id={axis: dev}, device_id_type=pl.DeviceIdType.MESH)

    def cols(k):
        return pl.ds(k * CW, CW)

    def st0(u):
        return copy_to(p_s.at[lax.rem(u, 2), 1 - me.c], q_s.at[lax.rem(u, QB)], s0_send.at[lax.rem(u, QB)], s0_recv.at[lax.rem(u, QB)], me.peer())

    def q_block(u, k, by):
        along = RINGS[k][0]
        q = q_s.at[lax.rem(u, QB)]
        b = me.block(along, by)
        return q.at[b, :, :, cols(k)] if along == "x" else q.at[:, b, :, cols(k)]

    def st1(u, k, s):
        along, _, sg = RINGS[k]
        rs = lax.rem(u, RB)
        src = q_block(u, k, -sg) if s == 0 else r1_s.at[rs, s - 1, k]
        return copy_to(src, r1_s.at[rs, s, k], s1_send.at[rs, s, k], s1_recv.at[rs, s, k], me.step(along, sg))

    def st2(u, k, s):
        _, along, sg = RINGS[k]
        rs = lax.rem(u, RB)
        src = r1_s.at[rs, n - 2, k, me.block(along, -sg)] if s == 0 else r2_s.at[rs, s - 1, k]
        return copy_to(src, r2_s.at[rs, s, k], s2_send.at[rs, s, k], s2_recv.at[rs, s, k], me.step(along, sg))

    def on_st0(u):
        st0(u).wait()
        qi, pi = lax.rem(u, QB), lax.rem(u, 2)

        def add(i, _):
            a, b = lax.div(i, n), lax.rem(i, n)
            q_s[qi, a, b] = q_s[qi, a, b] + p_s[pi, me.c, a, b]
            return 0
        lax.fori_loop(0, n * n, add, 0)
        for k in range(COLORS):
            st1(u, k, 0).start()

    def on_st1(u, s):
        for k in range(COLORS):
            st1(u, k, s).wait()
        rs = lax.rem(u, RB)
        for k in range(COLORS):
            sg = RINGS[k][2]
            own = q_block(u, k, -sg * (2 + s))

            def add(i, _, k=k, own=own):
                r1_s[rs, s, k, i] = r1_s[rs, s, k, i] + own[i]
                return 0
            lax.fori_loop(0, n, add, 0)
        for k in range(COLORS):
            (st1(u, k, s + 1) if s < n - 2 else st2(u, k, 0)).start()

    def shard_rows(u):
        r = u * 2 * TM + ((me.c * n + me.x) * n + me.y) * RR
        return pl.ds(pl.multiple_of(r, RR), RR)

    def fetch(u):
        return (pltpu.make_async_copy(xh_ref.at[shard_rows(u), :], fx_s, f_sem.at[0]),
                pltpu.make_async_copy(dyh_ref.at[shard_rows(u), :], fd_s, f_sem.at[1]))

    def put(u):
        return pltpu.make_async_copy(fo_s, sh_ref.at[u], fo_sem)

    def on_st2(u, s):
        for k in range(COLORS):
            st2(u, k, s).wait()
        rs = lax.rem(u, RB)
        for k in range(COLORS):
            along, sg = RINGS[k][1], RINGS[k][2]
            own = r1_s.at[rs, n - 2, k, me.block(along, -sg * (2 + s))]
            r2_s[rs, s, k] = r2_s[rs, s, k] + own[...]
            if s < n - 2:
                st2(u, k, s + 1).start()
        if s == n - 3:
            for f in fetch(u):
                f.start()
        if s == n - 2:
            for f in fetch(u):
                f.wait()

            @pl.when(u > 0)
            def _():
                put(u - 1).wait()
            xhat, r = normalize(fx_s[...])
            total = jnp.concatenate([r2_s[rs, s, k] for k in range(COLORS)], axis=-1).astype(F32)
            dh = total * g_ref[...]
            gx = r * (dh - jnp.mean(dh, axis=-1, keepdims=True) - xhat * jnp.mean(dh * xhat, axis=-1, keepdims=True))
            fo_s[...] = (fd_s[...].astype(F32) + gx).astype(BF)
            put(u).start()

            @pl.when(u == nu - 1)
            def _():
                put(u).wait()

    events = {2: on_st0}
    for s in range(n - 1):
        events[2 + 3 * (s + 1)] = functools.partial(on_st1, s=s)
        events[2 + 3 * (s + n)] = functools.partial(on_st2, s=s)

    def comm(r):
        for rho, fn in events.items():
            if rho % 4 != r:
                continue
            back = 2 + rho // 4
            u = lax.div(g - back, 2)

            @pl.when((g >= back) & (lax.rem(g - back + 2 * nt, 2) == 0) & (u < nu))
            def _():
                fn(u)

    def ln_block(src, dst_slot, r0, m):
        rows = pl.ds(pl.multiple_of(r0, m), m)
        xhat, _ = normalize(src[rows, :])
        ln_s[dst_slot, rows, :] = (xhat * g_ref[...] + b_ref[...]).astype(BF)

    def out_copy(sl, tt):
        return pltpu.make_async_copy(ln_s.at[sl], lnh_ref.at[pl.ds(pl.multiple_of(tt * TM, TM), TM), :], ln_sem.at[sl])

    @pl.when(g == 0)
    def _():
        me.greet()

        def lnb(i, _):
            ln_block(x0_ref, 0, i * 16, 16)
            return 0
        lax.fori_loop(0, TM // 16, lnb, 0)

    live = g < nt

    @pl.when((g > 0) & (g <= nt))
    def _():
        out_copy(nxt, g - 1).wait()

    comm(0)

    @pl.when(live)
    def _():
        out_copy(slot, g).start()
        lns = ln_s.at[slot]
        qkv_s[...] = dg(wt_ref[:C, :], lns[...], 1, 1).astype(BF)
        y = dg(wd_ref[:d + F // 2, :], dy_ref[...], 1, 1)
        do_s[...] = y[:d].astype(BF)
        da_s[:F // 2, :] = y[d:]

    comm(1)

    @pl.when(live)
    def _():
        lns = ln_s.at[slot]
        h_s[:F // 2, :] = dg(wt_ref[C:C + F // 2, :], lns[...], 1, 1)
        da_s[F // 2:, :] = dg(wd_ref[d + F // 2:, :], dy_ref[...], 1, 1)
        h_s[F // 2:, :] = dg(wt_ref[C + F // 2:, :], lns[...], 1, 1)
        for s in range(TM // S):
            cs = slice(s * S, (s + 1) * S)
            o, dq, dk, dv = attend(qkv_s[:d, cs], qkv_s[d:2 * d, cs], qkv_s[2 * d:3 * d, cs], do_s[:, cs], d ** -0.5)
            og_ref[:d, cs] = o
            dc_ref[:d, cs] = dq
            dc_ref[d:2 * d, cs] = dk
            dc_ref[2 * d:3 * d, cs] = dv

    comm(2)

    nsteps = D // NB
    LR = TM // nsteps
    uslot = lax.rem(lax.div(g, 2), 2)

    def c_block(i, _):
        cs = pl.ds(pl.multiple_of(i * NB, NB), NB)
        res = dg(dct_s[...], wt_ref[:, cs], 1, 0).astype(BF)
        p_s[uslot, slot, :, :, :, cs] = res.reshape(n, n, RR, NB)
        for j in range(LR // 16):
            ln_block(x_ref, nxt, i * LR + j * 16, 16)
        return 0

    @pl.when(live)
    def _():
        def gb(i, _):
            r = pl.ds(pl.multiple_of(i * 16, 16), 16)
            h = h_s[r, :]
            cdf = 0.5 * (1.0 + lax.erf(h * GELU_COEF))
            og_ref[pl.ds(pl.multiple_of(d + i * 16, 16), 16), :] = (h * cdf).astype(BF)
            dc_ref[pl.ds(pl.multiple_of(C + i * 16, 16), 16), :] = (da_s[r, :] * (cdf + h * PDF_COEF * jnp.exp(-0.5 * h * h))).astype(BF)
            return 0
        lax.fori_loop(0, F // 16, gb, 0, unroll=2)
        dct_s[...] = dc_ref[...].T
        lax.fori_loop(0, nsteps // 2, c_block, 0)

    comm(3)

    @pl.when(live)
    def _():
        lax.fori_loop(nsteps // 2, nsteps, c_block, 0)

    @pl.when(live & (slot == 1))
    def _():
        st0(lax.div(g, 2)).start()


def forward(axis, side, x, dy, gain, bias, wt, wd, S, TM=256, NB=1024):
    T, D = x.shape
    CF, dF = wt.shape[0], wd.shape[0]
    d = (CF - dF) // 2
    C = 3 * d
    F = CF - C
    nt = T // TM
    nu = nt // 2
    RR = 2 * TM // (CORES * side * side)
    drain = 2 + (2 + 3 * (2 * side - 2)) // 4 - 1
    CW = D // COLORS
    last = nt - 1
    QB, RB = 3, 4
    return pl.pallas_call(
        functools.partial(forward_kernel, axis, side, S, d, C, F, nt, NB),
        grid=(nt + drain,),
        in_specs=[pl.BlockSpec((TM, D), lambda t: (0, 0), pipeline_mode=pl.Buffered(1)),
                  pl.BlockSpec((TM, D), lambda t: (jnp.minimum(t + 1, last), 0)),
                  pl.BlockSpec((TM, D), lambda t: (jnp.minimum(t, last), 0)),
                  pl.BlockSpec((1, D), lambda t: (0, 0)),
                  pl.BlockSpec((1, D), lambda t: (0, 0)),
                  pl.BlockSpec((CF, D), lambda t: (0, 0), pipeline_mode=pl.Buffered(1)),
                  pl.BlockSpec((dF, D), lambda t: (0, 0), pipeline_mode=pl.Buffered(1)),
                  pl.BlockSpec(memory_space=pl.ANY),
                  pl.BlockSpec(memory_space=pl.ANY)],
        out_specs=[pl.BlockSpec(memory_space=pl.ANY),
                   pl.BlockSpec((CF, TM), lambda t: (0, jnp.minimum(t, last))),
                   pl.BlockSpec((dF, TM), lambda t: (0, jnp.minimum(t, last))),
                   pl.BlockSpec(memory_space=pl.ANY)],
        out_shape=[jax.ShapeDtypeStruct((T, D), BF), jax.ShapeDtypeStruct((CF, T), BF),
                   jax.ShapeDtypeStruct((dF, T), BF), jax.ShapeDtypeStruct((nu, RR, D), BF)],
        scratch_shapes=[pltpu.VMEM((2, TM, D), BF), pltpu.VMEM((F, TM), F32), pltpu.VMEM((F, TM), F32),
                        pltpu.VMEM((C, TM), BF), pltpu.VMEM((d, TM), BF), pltpu.VMEM((TM, CF), BF),
                        pltpu.VMEM((2, CORES, side, side, RR, D), BF),
                        pltpu.VMEM((QB, side, side, RR, D), BF),
                        pltpu.VMEM((RB, side - 1, COLORS, side, RR, CW), BF),
                        pltpu.VMEM((RB, side - 1, COLORS, RR, CW), BF),
                        pltpu.VMEM((RR, D), BF), pltpu.VMEM((RR, D), BF), pltpu.VMEM((RR, D), BF),
                        pltpu.SemaphoreType.DMA((2,)),
                        pltpu.SemaphoreType.DMA((QB,)), pltpu.SemaphoreType.DMA((QB,)),
                        pltpu.SemaphoreType.DMA((RB, side - 1, COLORS)), pltpu.SemaphoreType.DMA((RB, side - 1, COLORS)),
                        pltpu.SemaphoreType.DMA((RB, side - 1, COLORS)), pltpu.SemaphoreType.DMA((RB, side - 1, COLORS)),
                        pltpu.SemaphoreType.DMA((2,)), pltpu.SemaphoreType.DMA],
        compiler_params=pltpu.CompilerParams(vmem_limit_bytes=VMEM_LIMIT, collective_id=1, has_side_effects=True),
        name="forward_rs",
    )(x, x, dy, gain.reshape(1, D), bias.reshape(1, D), wt, wd, x, dy)


def gather_kernel(axis, side, NP, sh_ref, dc_ref, ln_ref, o_ref, g_ref, own_s, l_sem, snd, rcv, p_snd, p_rcv):
    n = side
    me = Place(axis, side)
    g = pl.program_id(0)
    ng = 8
    nu, RR, D = sh_ref.shape
    PU = nu // NP
    CW = D // COLORS
    HA = n - 1

    def copy_to(src, dst, ssem, rsem, dev):
        return pltpu.make_async_remote_copy(src_ref=src, dst_ref=dst, send_sem=ssem, recv_sem=rsem,
                                            device_id={axis: dev}, device_id_type=pl.DeviceIdType.MESH)

    def units(p):
        return pl.ds(p * PU, PU)

    def region(p, k, h, lag):
        along_b, along_a, sg = RINGS[k]
        cw = pl.ds(k * CW, CW)
        if h < HA:
            b = me.block(along_a, -sg * lag)
            xi, yi = (me.x, b) if along_a == "y" else (b, me.y)
            return g_ref.at[units(p), me.c, xi, yi, :, cw]
        b = me.block(along_b, -sg * lag)
        if along_b == "x":
            return g_ref.at[units(p), me.c, b, :, :, cw]
        return g_ref.at[units(p), me.c, :, b, :, cw]

    def hop(p, k, h):
        along_b, along_a, sg = RINGS[k]
        s = h if h < HA else h - HA
        dst = region(p, k, h, s)
        src = own_s.at[units(p), :, pl.ds(k * CW, CW)] if h == 0 else dst
        return copy_to(src, dst, snd.at[p, k, h], rcv.at[p, k, h], me.step(along_a if h < HA else along_b, sg))

    def to_peer(src, dst):
        return copy_to(src, dst, p_snd, p_rcv, me.peer())

    def arrived(p, h):
        for k in range(COLORS):
            hop(p, k, h).wait()
            if h < 2 * HA - 1:
                hop(p, k, h + 1).start()
            s = h if h < HA else h - HA
            got = region(p, k, h, s + 1)
            to_peer(got, got).start()

    def mine():
        return g_ref.at[:, me.c, me.x, me.y]

    @pl.when(g == 0)
    def _():
        me.greet()
        ld = pltpu.make_async_copy(sh_ref, own_s, l_sem)
        ld.start()
        ld.wait()
        for p in range(NP):
            for k in range(COLORS):
                hop(p, k, 0).start()
        pltpu.make_async_copy(own_s, mine(), l_sem).start()
        to_peer(own_s, mine()).start()

    M = dc_ref.shape[0]
    half = M // 2
    for j in range(2):
        rows = slice(j * half, (j + 1) * half)
        o_ref[rows, :] = jnp.dot(dc_ref[rows, :], ln_ref[...], preferred_element_type=F32).astype(BF)
        if j == 0:
            @pl.when(g == 0)
            def _():
                pltpu.make_async_copy(own_s, mine(), l_sem).wait()
        for h in range(HA):
            @pl.when(g == h)
            def _(h=h):
                arrived(2 * j, h)
                arrived(2 * j + 1, h)

        @pl.when((g == 3) | (g == 4))
        def _():
            arrived(2 * (g - 3) + j, 3)

        @pl.when(g == 5)
        def _():
            arrived(2 * j, 4)
            arrived(2 * j + 1, 4)

        @pl.when((g == 6) | (g == 7))
        def _():
            arrived(2 * (g - 6) + j, 5)

    @pl.when(g == ng - 1)
    def _():
        to_peer(g_ref.at[:, me.c], g_ref.at[:, me.c]).wait()


def gather(axis, side, sh, dc, ln, NB=512):
    nu, RR, D = sh.shape
    M, T = dc.shape
    NP = 4
    hops = 2 * (side - 1)
    return pl.pallas_call(
        functools.partial(gather_kernel, axis, side, NP),
        grid=(D // NB,),
        in_specs=[pl.BlockSpec(memory_space=pl.ANY),
                  pl.BlockSpec((M, T), lambda t: (0, 0), pipeline_mode=pl.Buffered(1)),
                  pl.BlockSpec((T, NB), lambda t: (0, t))],
        out_specs=[pl.BlockSpec((M, NB), lambda t: (0, t)), pl.BlockSpec(memory_space=pl.ANY)],
        out_shape=[jax.ShapeDtypeStruct((M, D), BF), jax.ShapeDtypeStruct((nu, CORES, side, side, RR, D), BF)],
        scratch_shapes=[pltpu.VMEM((nu, RR, D), BF), pltpu.SemaphoreType.DMA,
                        pltpu.SemaphoreType.DMA((NP, COLORS, hops)), pltpu.SemaphoreType.DMA((NP, COLORS, hops)),
                        pltpu.SemaphoreType.DMA, pltpu.SemaphoreType.DMA],
        compiler_params=pltpu.CompilerParams(vmem_limit_bytes=VMEM_LIMIT, collective_id=2, has_side_effects=True),
        name="gather_grads",
    )(sh, dc, ln)


def finish_kernel(d, C, og_ref, dy_ref, ot_ref, gh_ref, gw_ref, gd_ref, gq_ref, gu_ref, dx_ref, buf, isem, osem):
    g = pl.program_id(0)
    ng = pl.num_programs(0)
    R = buf.shape[1]

    def cin(a):
        return pltpu.make_async_copy(gh_ref.at[pl.ds(pl.multiple_of(a * R, R), R), :], buf.at[lax.rem(a, 4)], isem.at[lax.rem(a, 4)])

    def cout(a):
        return pltpu.make_async_copy(buf.at[lax.rem(a, 4)], dx_ref.at[pl.ds(pl.multiple_of(a * R, R), R), :], osem.at[lax.rem(a, 4)])

    @pl.when(g == 0)
    def _():
        cin(0).start()
        cin(1).start()
    for j in range(2):
        a = 2 * g + j
        cin(a).wait()
        cout(a).start()

        @pl.when(g > 0)
        def _():
            cout(a - 2).wait()

        @pl.when(g < ng - 1)
        def _():
            cin(a + 2).start()
    res = jnp.dot(og_ref[...], dy_ref[...], preferred_element_type=F32).astype(BF)
    gw_ref[...] = res[:d]
    gd_ref[...] = res[d:]
    gq_ref[...] = ot_ref[:C, :].T
    gu_ref[...] = ot_ref[C:, :].T

    @pl.when(g == ng - 1)
    def _():
        cout(2 * g).wait()
        cout(2 * g + 1).wait()


def finish(d, C, og, dy, ot, gathered, NB=512):
    M, T = og.shape
    D = dy.shape[1]
    CF = ot.shape[0]
    steps = D // NB
    R = T // (2 * steps)
    return pl.pallas_call(
        functools.partial(finish_kernel, d, C),
        grid=(steps,),
        in_specs=[pl.BlockSpec((M, T), lambda t: (0, 0), pipeline_mode=pl.Buffered(1)),
                  pl.BlockSpec((T, NB), lambda t: (0, t)),
                  pl.BlockSpec((CF, NB), lambda t: (0, t)),
                  pl.BlockSpec(memory_space=pl.ANY)],
        out_specs=[pl.BlockSpec((d, NB), lambda t: (0, t)), pl.BlockSpec((M - d, NB), lambda t: (0, t)),
                   pl.BlockSpec((NB, C), lambda t: (t, 0)), pl.BlockSpec((NB, CF - C), lambda t: (t, 0)),
                   pl.BlockSpec(memory_space=pl.ANY)],
        out_shape=[jax.ShapeDtypeStruct((d, D), BF), jax.ShapeDtypeStruct((M - d, D), BF),
                   jax.ShapeDtypeStruct((D, C), BF), jax.ShapeDtypeStruct((D, CF - C), BF),
                   jax.ShapeDtypeStruct((T, D), BF)],
        scratch_shapes=[pltpu.VMEM((4, R, D), BF), pltpu.SemaphoreType.DMA((4,)), pltpu.SemaphoreType.DMA((4,))],
        compiler_params=pltpu.CompilerParams(vmem_limit_bytes=VMEM_LIMIT),
        name="finish_grads",
    )(og, dy, ot, gathered)


def solution(mesh):
    row_spec = P('dp', None, None)
    in_specs = (row_spec, P(None), P(None), P(None, 'tp', None), P('tp', None), P(None, 'tp'), P('tp', None), row_spec)
    out_specs = (row_spec, P('dp', 'tp', None), P(('dp', 'tp'), None), P('dp', 'tp'), P(('dp', 'tp'), None))
    chips = mesh.shape['tp'] // CORES
    side = int(round(chips ** 0.5))
    assert side * side == chips

    def device_step(tokens, ln_gain, ln_bias, w_qkv, w_out, w_up, w_down, grad_out):
        rows, seq, D = tokens.shape
        T = rows * seq
        C = w_qkv.shape[1] * w_qkv.shape[2]
        d = w_out.shape[0]
        x = tokens.reshape(T, D)
        dy = grad_out.reshape(T, D)
        wt = jnp.concatenate([w_qkv.reshape(D, C).T, w_up.T], axis=0)
        wd = jnp.concatenate([w_out, w_down], axis=0)
        ln, dc, og, sh = forward('tp', side, x, dy, ln_gain, ln_bias, wt, wd, seq)
        ot, gathered = gather('tp', side, sh, dc, ln)
        gw, gd, gq, gu, dx = finish(d, C, og, dy, ot, gathered.reshape(T, D))
        return dx.reshape(tokens.shape), gq.reshape(w_qkv.shape), gw, gu, gd

    return jax.shard_map(device_step, mesh=mesh, in_specs=in_specs, out_specs=out_specs, check_vma=False)
```

```python
import functools
import jax
import jax.numpy as jnp
from jax import lax
from jax.experimental import pallas as pl
from jax.experimental.pallas import tpu as pltpu
from jax.sharding import PartitionSpec as P

EPS = 1e-5
GELU_COEF = 0.7071067811865476
PDF_COEF = 0.3989422804014327
F32 = jnp.float32
BF = jnp.bfloat16
VMEM_LIMIT = 64 * 2**20 - 65536
CORES = 2
COLORS = 4
AG_EVERY = 24
NB = 512


def dg(a, b, ca, cb):
    return lax.dot_general(a, b, (((ca,), (cb,)), ((), ())), preferred_element_type=F32)


def normalize(x):
    x = x.astype(F32)
    c = x - jnp.mean(x, axis=-1, keepdims=True)
    r = lax.rsqrt(jnp.mean(c * c, axis=-1, keepdims=True) + EPS)
    return c * r, r


def ln_rows(x_ref, dst, rows, g_ref, b_ref, CH=512):
    D = x_ref.shape[1]
    tot = sq = None
    for c in range(0, D, CH):
        v = jnp.sum(x_ref[rows, c:c + CH].astype(F32), axis=-1, keepdims=True)
        tot = v if tot is None else tot + v
    mean = tot * (1.0 / D)
    for c in range(0, D, CH):
        v = x_ref[rows, c:c + CH].astype(F32) - mean
        v = jnp.sum(v * v, axis=-1, keepdims=True)
        sq = v if sq is None else sq + v
    r = lax.rsqrt(sq * (1.0 / D) + EPS)
    for c in range(0, D, CH):
        v = x_ref[rows, c:c + CH].astype(F32) - mean
        dst[rows, c:c + CH] = (v * r * g_ref[:, c:c + CH] + b_ref[:, c:c + CH]).astype(BF)


class Tile:
    def __init__(self, ln, dy, wt, wd, dct, qkv_s, do_s, h_s, da_s, og_ref, dc_ref, st_s, dp_s, p_b, ds_b, C, F, d, store):
        self.ln, self.dy, self.wt, self.wd, self.dct = ln, dy, wt, wd, dct
        self.qkv_s, self.do_s, self.h_s, self.da_s = qkv_s, do_s, h_s, da_s
        self.og_ref, self.dc_ref, self.st_s, self.dp_s, self.p_b, self.ds_b = og_ref, dc_ref, st_s, dp_s, p_b, ds_b
        self.C, self.F, self.d, self.store = C, F, d, store
        self.S, self.D = ln.shape

    def project(self, side, pieces):
        wt, wd, C, d, half = self.wt, self.wd, self.C, self.d, self.F // 2

        def more(j):
            for i in range(pieces * j // 5, pieces * (j + 1) // 5):
                side(i)
        self.qkv_s[...] = dg(wt[:C, :], self.ln[...], 1, 1).astype(BF)
        more(0)
        y = dg(wd[:d + half, :], self.dy[...], 1, 1)
        self.do_s[...] = y[:d].astype(BF)
        self.da_s[:half, :] = y[d:]
        more(1)
        self.h_s[:half, :] = dg(wt[C:C + half, :], self.ln[...], 1, 1)
        more(2)
        self.da_s[half:, :] = dg(wd[d + half:, :], self.dy[...], 1, 1)
        more(3)
        self.h_s[half:, :] = dg(wt[C + half:, :], self.ln[...], 1, 1)
        more(4)

    def col(self, i):
        self.store(i, dg(self.dct[...], self.wt[:, i * NB:(i + 1) * NB], 1, 0).astype(BF))

    def gelu(self, i, n):
        for j in range(2):
            r0 = (2 * i + j) * n
            h = self.h_s[r0:r0 + n, :]
            cdf = 0.5 * (1.0 + lax.erf(h * GELU_COEF))
            self.og_ref[self.d + r0:self.d + r0 + n, :] = (h * cdf).astype(BF)
            slope = cdf + h * PDF_COEF * jnp.exp(-0.5 * h * h)
            self.dc_ref[self.C + r0:self.C + r0 + n, :] = (self.da_s[r0:r0 + n, :] * slope).astype(BF)

    def softmax(self, scale, QC=128):
        S = self.S
        for c in range(0, S, QC):
            kk = c + QC
            qs = slice(c, c + QC)
            st = self.st_s[:kk, qs] * scale
            ki = lax.broadcasted_iota(jnp.int32, (kk, QC), 0)
            qi = lax.broadcasted_iota(jnp.int32, (kk, QC), 1) + c
            st = jnp.where(ki <= qi, st, -1e30)
            e = jnp.exp(st - jnp.max(st, axis=0, keepdims=True))
            p = e / jnp.sum(e, axis=0, keepdims=True)
            dp = self.dp_s[:kk, qs]
            rd = jnp.sum(p * dp, axis=0, keepdims=True)
            self.p_b[:kk, qs] = p.astype(BF)
            self.ds_b[:kk, qs] = (p * (dp - rd) * scale).astype(BF)
            if kk < S:
                self.p_b[kk:, qs] = jnp.zeros((S - kk, QC), BF)
                self.ds_b[kk:, qs] = jnp.zeros((S - kk, QC), BF)

    def rest(self):
        d = self.d
        scale = d ** -0.5
        n = self.D // NB
        rows = self.F // (2 * n)
        q, k, v, do = self.qkv_s[:d, :], self.qkv_s[d:2 * d, :], self.qkv_s[2 * d:3 * d, :], self.do_s[...]
        self.col(0)
        self.st_s[...] = dg(k, q, 0, 0)
        self.dp_s[...] = dg(v, do, 0, 0)
        self.col(1)
        self.gelu(0, rows)
        self.gelu(1, rows)
        self.softmax(scale)
        self.col(2)
        self.gelu(2, rows)
        self.og_ref[:d, :] = dg(v, self.p_b[...], 1, 0).astype(BF)
        self.dc_ref[2 * d:3 * d, :] = dg(do, self.p_b[...], 1, 1).astype(BF)
        self.col(3)
        self.gelu(3, rows)
        self.dc_ref[:d, :] = dg(k, self.ds_b[...], 1, 0).astype(BF)
        self.dc_ref[d:2 * d, :] = dg(q, self.ds_b[...], 1, 1).astype(BF)
        for i in range(4, n):
            self.col(i)
            self.gelu(i, rows)
        self.dct[...] = self.dc_ref[...].T

    def last(self):
        for i in range(self.D // NB):
            self.col(i)


class Place:
    def __init__(self, axis, side):
        self.axis, self.side = axis, side
        i = lax.axis_index(axis)
        self.c = lax.rem(i, CORES)
        chip = lax.div(i, CORES)
        x, y = lax.rem(chip, side), lax.div(chip, side)
        self.at = {"x": [x] + [lax.rem(x + j, side) for j in range(1, side)],
                   "y": [y] + [lax.rem(y + j, side) for j in range(1, side)]}
        self.x, self.y = x, y
        self.next = {}
        for sg in (1, -1):
            self.next["x", sg] = self.index(self.block("x", sg), y, self.c)
            self.next["y", sg] = self.index(x, self.block("y", sg), self.c)
        self.other = self.index(x, y, 1 - self.c)

    def index(self, x, y, c):
        return (y * self.side + x) * CORES + c

    def step(self, along, by):
        return self.next[along, by]

    def peer(self):
        return self.other

    def block(self, along, by):
        return self.at[along][by % self.side]

    def partners(self):
        return [self.step("x", 1), self.step("x", -1), self.step("y", 1), self.step("y", -1), self.peer()]

    def greet(self):
        sem = pltpu.get_barrier_semaphore()
        who = self.partners()
        for w in who:
            pl.semaphore_signal(sem, inc=1, device_id={self.axis: w}, device_id_type=pl.DeviceIdType.MESH)
        pl.semaphore_wait(sem, len(who))


RINGS = (("x", "y", 1), ("x", "y", -1), ("y", "x", 1), ("y", "x", -1))


class Gather:
    def __init__(self, me, g_ref, own, base, PU, snd, rcv, p_snd, p_rcv, own_sem):
        self.me, self.g, self.own, self.base, self.PU = me, g_ref, own, base, PU
        self.snd, self.rcv, self.p_snd, self.p_rcv, self.own_sem = snd, rcv, p_snd, p_rcv, own_sem
        self.HA = me.side - 1
        self.CW = g_ref.shape[-1] // COLORS

    def send(self, src, dst, ssem, rsem, dev):
        return pltpu.make_async_remote_copy(src_ref=src, dst_ref=dst, send_sem=ssem, recv_sem=rsem,
                                            device_id={self.me.axis: dev}, device_id_type=pl.DeviceIdType.MESH)

    def units(self, p):
        return pl.ds(self.base + p * self.PU, self.PU)

    def region(self, p, k, h, lag):
        me = self.me
        along_b, along_a, sg = RINGS[k]
        cw = pl.ds(k * self.CW, self.CW)
        if h < self.HA:
            b = me.block(along_a, -sg * lag)
            xi, yi = (me.x, b) if along_a == "y" else (b, me.y)
            return self.g.at[self.units(p), me.c, xi, yi, :, cw]
        b = me.block(along_b, -sg * lag)
        if along_b == "x":
            return self.g.at[self.units(p), me.c, b, :, :, cw]
        return self.g.at[self.units(p), me.c, :, b, :, cw]

    def hop(self, p, k, h):
        along_b, along_a, sg = RINGS[k]
        dst = self.region(p, k, h, h if h < self.HA else h - self.HA)
        src = self.own.at[pl.ds(p * self.PU, self.PU), :, pl.ds(k * self.CW, self.CW)] if h == 0 else dst
        return self.send(src, dst, self.snd.at[p, k, h], self.rcv.at[p, k, h],
                         self.me.step(along_a if h < self.HA else along_b, sg))

    def mine(self, p):
        return self.g.at[self.units(p), self.me.c, self.me.x, self.me.y]

    def keep(self, p):
        return pltpu.make_async_copy(self.own.at[pl.ds(p * self.PU, self.PU)], self.mine(p), self.own_sem.at[p])

    def to_peer(self, src, dst):
        return self.send(src, dst, self.p_snd, self.p_rcv, self.me.peer())

    def begin(self, p):
        for k in range(COLORS):
            self.hop(p, k, 0).start()
        self.keep(p).start()
        self.to_peer(self.own.at[pl.ds(p * self.PU, self.PU)], self.mine(p)).start()

    def arrived(self, p, h):
        HA = self.HA
        if h == HA - 1:
            self.keep(p).wait()
        for k in range(COLORS):
            self.hop(p, k, h).wait()
            if h < 2 * HA - 1:
                self.hop(p, k, h + 1).start()
            got = self.region(p, k, h, (h if h < HA else h - HA) + 1)
            self.to_peer(got, got).start()

    def end(self, count):
        every = self.g.at[pl.ds(self.base, count * self.PU), self.me.c]
        self.to_peer(every, every).wait()


def forward_kernel(axis, side, S, d, C, F, nt, PU, early,
                   x0_ref, x_ref, dy_ref, g_ref, b_ref, wqh_ref, wuh_ref, woh_ref, wdh_ref, xh_ref, dyh_ref,
                   lnh_ref, dc_ref, og_ref, sh_ref, gat_ref,
                   wt_ref, wd_ref, wq_s, wu_s, ln_s, h_s, da_s, qkv_s, do_s, dct_s, st_s, dp_s, p_b, ds_b, p_s, q_s, r1_s, r2_s, fx_s, fd_s, fo_s,
                   w_sem, wst_sem, ln_sem, s0_send, s0_recv, s1_send, s1_recv, s2_send, s2_recv, f_sem, fo_sem,
                   a_send, a_recv, ap_send, ap_recv, ao_sem):
    TM, D = x_ref.shape
    n = side
    me = Place(axis, side)
    g = pl.program_id(0)
    slot = lax.rem(g, 2)
    nxt = 1 - slot
    nu = nt // 2
    CW = D // COLORS
    QB = q_s.shape[0]
    RB = r1_s.shape[0]
    RR = q_s.shape[3]

    def copy_to(src, dst, ssem, rsem, dev):
        return pltpu.make_async_remote_copy(src_ref=src, dst_ref=dst, send_sem=ssem, recv_sem=rsem,
                                            device_id={axis: dev}, device_id_type=pl.DeviceIdType.MESH)

    def cols(k):
        return pl.ds(k * CW, CW)

    def st0(u):
        return copy_to(p_s.at[lax.rem(u, 2), 1 - me.c], q_s.at[lax.rem(u, QB)], s0_send.at[lax.rem(u, QB)], s0_recv.at[lax.rem(u, QB)], me.peer())

    def q_block(u, k, by):
        along = RINGS[k][0]
        q = q_s.at[lax.rem(u, QB)]
        b = me.block(along, by)
        return q.at[b, :, :, cols(k)] if along == "x" else q.at[:, b, :, cols(k)]

    def st1(u, k, s):
        along, _, sg = RINGS[k]
        rs = lax.rem(u, RB)
        src = q_block(u, k, -sg) if s == 0 else r1_s.at[rs, s - 1, k]
        return copy_to(src, r1_s.at[rs, s, k], s1_send.at[rs, s, k], s1_recv.at[rs, s, k], me.step(along, sg))

    def st2(u, k, s):
        _, along, sg = RINGS[k]
        rs = lax.rem(u, RB)
        src = r1_s.at[rs, n - 2, k, me.block(along, -sg)] if s == 0 else r2_s.at[rs, s - 1, k]
        return copy_to(src, r2_s.at[rs, s, k], s2_send.at[rs, s, k], s2_recv.at[rs, s, k], me.step(along, sg))

    def on_st0(u):
        st0(u).wait()
        qi, pi = lax.rem(u, QB), lax.rem(u, 2)

        for a in range(n):
            for b in range(n):
                q_s[qi, a, b] = q_s[qi, a, b] + p_s[pi, me.c, a, b]
        for k in range(COLORS):
            st1(u, k, 0).start()

    def on_st1(u, s):
        for k in range(COLORS):
            st1(u, k, s).wait()
        rs = lax.rem(u, RB)
        for k in range(COLORS):
            sg = RINGS[k][2]
            own = q_block(u, k, -sg * (2 + s))

            r1_s[rs, s, k] = r1_s[rs, s, k] + own[...]
        for k in range(COLORS):
            (st1(u, k, s + 1) if s < n - 2 else st2(u, k, 0)).start()

    def shard_rows(u):
        r = u * 2 * TM + ((me.c * n + me.x) * n + me.y) * RR
        return pl.ds(pl.multiple_of(r, RR), RR)

    def fetch(u):
        return (pltpu.make_async_copy(xh_ref.at[shard_rows(u), :], fx_s, f_sem.at[0]),
                pltpu.make_async_copy(dyh_ref.at[shard_rows(u), :], fd_s, f_sem.at[1]))

    UE = early * PU
    ag = Gather(me, gat_ref, fo_s, 0, PU, a_send, a_recv, ap_send, ap_recv, ao_sem)

    def put(u):
        return pltpu.make_async_copy(fo_s.at[UE + lax.rem(u, 2)], sh_ref.at[u - UE], fo_sem.at[lax.rem(u, 2)])

    def on_st2(u, s):
        for k in range(COLORS):
            st2(u, k, s).wait()
        rs = lax.rem(u, RB)
        for k in range(COLORS):
            along, sg = RINGS[k][1], RINGS[k][2]
            own = r1_s.at[rs, n - 2, k, me.block(along, -sg * (2 + s))]
            r2_s[rs, s, k] = r2_s[rs, s, k] + own[...]
            if s < n - 2:
                st2(u, k, s + 1).start()
        if s == n - 3:
            for f in fetch(u):
                f.start()
        if s == n - 2:
            for f in fetch(u):
                f.wait()

            xhat, r = normalize(fx_s[...])
            total = jnp.concatenate([r2_s[rs, s, k] for k in range(COLORS)], axis=-1).astype(F32)
            dh = total * g_ref[...]
            gx = r * (dh - jnp.mean(dh, axis=-1, keepdims=True) - xhat * jnp.mean(dh * xhat, axis=-1, keepdims=True))
            done = (fd_s[...].astype(F32) + gx).astype(BF)

            @pl.when(u < UE)
            def _():
                fo_s[u] = done

            @pl.when((u < UE) & (lax.rem(u, PU) == PU - 1))
            def _():
                ag.begin(lax.div(u, PU))

            @pl.when(u >= UE + 2)
            def _():
                put(u - 2).wait()

            @pl.when(u >= UE)
            def _():
                fo_s[UE + lax.rem(u, 2)] = done
                put(u).start()

            @pl.when(u == nu - 1)
            def _():
                put(u - 1).wait()
                put(u).wait()

    rs_at = (4, 10, 16, 22, 26, 30, 34)
    ag_at = (6, 10, 14, 22, 30, 38)
    steps = [on_st0] + [functools.partial(on_st1, s=s) for s in range(n - 1)] + [functools.partial(on_st2, s=s) for s in range(n - 1)]

    def comm(r):
        now = 4 * g + r
        for rho, fn in reversed(list(zip(rs_at, steps, strict=True))):
            if rho % 4 != r:
                continue
            back = 3 + rho // 4
            u = lax.div(g - back, 2)

            @pl.when((g >= back) & (lax.rem(g - back + 2 * nt, 2) == 0) & (u < nu))
            def _():
                fn(u)
        for h, o in enumerate(ag_at):
            first = 8 * (PU - 1) + 12 + rs_at[-1] + o
            if first % 4 != r:
                continue
            p = lax.div(now - first, AG_EVERY)

            @pl.when((now >= first) & (lax.rem(now - first + 64 * AG_EVERY, AG_EVERY) == 0) & (p < early))
            def _():
                ag.arrived(p, h)

    def out_copy(sl, tt):
        return pltpu.make_async_copy(ln_s.at[sl], lnh_ref.at[pl.ds(pl.multiple_of(tt * TM, TM), TM), :], ln_sem.at[sl])

    @pl.when(g == 0)
    def _():
        WR = wq_s.shape[1]

        def w_in(i):
            rows = pl.ds(pl.multiple_of(i * WR, WR), WR)
            j = lax.rem(i, 2)
            return (pltpu.make_async_copy(wqh_ref.at[rows, :], wq_s.at[j], wst_sem.at[j, 0]),
                    pltpu.make_async_copy(wuh_ref.at[rows, :], wu_s.at[j], wst_sem.at[j, 1]))
        whole = (pltpu.make_async_copy(woh_ref, wd_ref.at[pl.ds(0, d), :], w_sem.at[0]),
                 pltpu.make_async_copy(wdh_ref, wd_ref.at[pl.ds(d, F), :], w_sem.at[1]))
        for cp in w_in(0) + w_in(1) + whole:
            cp.start()
        me.greet()

        dct_s[...] = jnp.zeros_like(dct_s)

        def lnb(i, _):
            ln_rows(x0_ref, ln_s.at[0], pl.ds(pl.multiple_of(i * 16, 16), 16), g_ref, b_ref)
            return 0
        lax.fori_loop(0, TM // 16, lnb, 0)

        def wtb(i, _):
            for cp in w_in(i):
                cp.wait()
            to = pl.ds(pl.multiple_of(i * WR, WR), WR)
            j = lax.rem(i, 2)
            wt_ref[:C, to] = wq_s[j].T
            wt_ref[C:, to] = wu_s[j].T

            @pl.when(i + 2 < D // WR)
            def _():
                for cp in w_in(i + 2):
                    cp.start()
            return 0
        lax.fori_loop(0, D // WR, wtb, 0)
        for cp in whole:
            cp.wait()

    live = g < nt

    @pl.when((g > 0) & (g <= nt))
    def _():
        out_copy(nxt, g - 1).wait()

    before = g + 3

    def store(i, v):
        p_s[lax.rem(lax.div(before, 2), 2), lax.rem(before, 2), :, :, :, pl.ds(i * NB, NB)] = v.reshape(n, n, RR, NB)
    tile = Tile(ln_s.at[slot], dy_ref, wt_ref, wd_ref, dct_s, qkv_s, do_s, h_s, da_s,
                og_ref, dc_ref, st_s, dp_s, p_b, ds_b, C, F, d, store)

    comm(0)

    @pl.when(live)
    def _():
        out_copy(slot, g).start()
        tile.project(lambda i: ln_rows(x_ref, ln_s.at[nxt], pl.ds(i * 8, 8), g_ref, b_ref), TM // 8)

    comm(2)

    @pl.when(live)
    def _():
        tile.rest()

    @pl.when(g == nt)
    def _():
        tile.last()

    @pl.when((g > 0) & (g <= nt) & (slot == 0))
    def _():
        st0(lax.div(g, 2) - 1).start()

    @pl.when(g == pl.num_programs(0) - 1)
    def _():
        ag.end(early)


def forward(axis, side, x, dy, gain, bias, w_qkv, w_up, w_out, w_down, S, TM=256, PU=2, early=2):
    T, D = x.shape
    C, F, d = w_qkv.shape[1], w_up.shape[1], w_out.shape[0]
    CF, dF = C + F, d + F
    nt = T // TM
    nu = nt // 2
    RR = 2 * TM // (CORES * side * side)
    drain = 10
    CW = D // COLORS
    last = nt - 1
    QB, RB, WR = 4, 5, 512
    UE = early * PU
    hops = 2 * (side - 1)
    dma = pltpu.SemaphoreType.DMA
    anyspace = pl.BlockSpec(memory_space=pl.ANY)
    return pl.pallas_call(
        functools.partial(forward_kernel, axis, side, S, d, C, F, nt, PU, early),
        grid=(nt + drain,),
        in_specs=[pl.BlockSpec((TM, D), lambda t: (0, 0), pipeline_mode=pl.Buffered(1)),
                  pl.BlockSpec((TM, D), lambda t: (jnp.minimum(t + 1, last), 0)),
                  pl.BlockSpec((TM, D), lambda t: (jnp.minimum(t, last), 0)),
                  pl.BlockSpec((1, D), lambda t: (0, 0)),
                  pl.BlockSpec((1, D), lambda t: (0, 0))] + [anyspace] * 6,
        out_specs=[anyspace,
                   pl.BlockSpec((CF, TM), lambda t: (0, jnp.minimum(t, last))),
                   pl.BlockSpec((dF, TM), lambda t: (0, jnp.minimum(t, last))),
                   anyspace, anyspace],
        out_shape=[jax.ShapeDtypeStruct((T, D), BF), jax.ShapeDtypeStruct((CF, T), BF),
                   jax.ShapeDtypeStruct((dF, T), BF), jax.ShapeDtypeStruct((nu - UE, RR, D), BF),
                   jax.ShapeDtypeStruct((nu, CORES, side, side, RR, D), BF)],
        scratch_shapes=[pltpu.VMEM((CF, D), BF), pltpu.VMEM((dF, D), BF),
                        pltpu.VMEM((2, WR, C), BF), pltpu.VMEM((2, WR, F), BF),
                        pltpu.VMEM((2, TM, D), BF), pltpu.VMEM((F, TM), F32), pltpu.VMEM((F, TM), F32),
                        pltpu.VMEM((C, TM), BF), pltpu.VMEM((d, TM), BF), pltpu.VMEM((TM, CF), BF),
                        pltpu.VMEM((S, S), F32), pltpu.VMEM((S, S), F32), pltpu.VMEM((S, S), BF), pltpu.VMEM((S, S), BF),
                        pltpu.VMEM((2, CORES, side, side, RR, D), BF),
                        pltpu.VMEM((QB, side, side, RR, D), BF),
                        pltpu.VMEM((RB, side - 1, COLORS, side, RR, CW), BF),
                        pltpu.VMEM((RB, side - 1, COLORS, RR, CW), BF),
                        pltpu.VMEM((RR, D), BF), pltpu.VMEM((RR, D), BF), pltpu.VMEM((UE + 2, RR, D), BF),
                        dma((2,)), dma((2, 2)), dma((2,)), dma((QB,)), dma((QB,)),
                        dma((RB, side - 1, COLORS)), dma((RB, side - 1, COLORS)),
                        dma((RB, side - 1, COLORS)), dma((RB, side - 1, COLORS)),
                        dma((2,)), dma((2,)),
                        dma((early, COLORS, hops)), dma((early, COLORS, hops)), dma, dma, dma((early,))],
        compiler_params=pltpu.CompilerParams(vmem_limit_bytes=VMEM_LIMIT, collective_id=1, has_side_effects=True),
        name="forward_rs",
    )(x, x, dy, gain.reshape(1, D), bias.reshape(1, D), w_qkv, w_up, w_out, w_down, x, dy)


def gather_kernel(axis, side, base, PU, sh_ref, dc_ref, og_ref, ln_ref, dy_ref, gin_ref, o1_ref, o2_ref, g_ref,
                  own_s, dc_s, og_s, l_sem, dc_sem, og_sem, snd, rcv, p_snd, p_rcv, own_sem):
    me = Place(axis, side)
    g = pl.program_id(0)
    ng = pl.num_programs(0)
    nl = sh_ref.shape[0]
    NP = nl // PU
    HA = side - 1
    M1, M2 = dc_s.shape[0] // 2, og_s.shape[0] // 2
    ag = Gather(me, g_ref, own_s, base, PU, snd, rcv, p_snd, p_rcv, own_sem)

    def left(j):
        src, dst, sem, M = ((dc_ref, dc_s, dc_sem, M1), (og_ref, og_s, og_sem, M2))[j // 2]
        rows = pl.ds((j % 2) * M, M)
        return pltpu.make_async_copy(src.at[rows, :], dst.at[rows, :], sem.at[j % 2])

    @pl.when(g == 0)
    def _():
        ld = pltpu.make_async_copy(sh_ref, own_s, l_sem)
        ld.start()
        left(0).start()
        me.greet()
        ld.wait()
        for p in range(NP):
            ag.begin(p)
        left(1).start()
        left(2).start()
        left(3).start()

    for j in range(2):
        @pl.when(g == 0)
        def _():
            left(2 * j).wait()
            left(2 * j + 1).wait()
        src, rhs, o_ref, M = ((dc_s, ln_ref, o1_ref, M1), (og_s, dy_ref, o2_ref, M2))[j]
        for i in range(2):
            rows = pl.ds(i * M, M)
            o_ref[rows, :] = jnp.dot(src[rows, :], rhs[...], preferred_element_type=F32).astype(BF)
        now = 2 * g + j
        half = -(-NP // 2)
        for h in range(HA):
            for i in range(half):
                p = lax.rem(now, 2) * half + i

                @pl.when((lax.div(now, 2) == h) & (p < NP))
                def _():
                    ag.arrived(p, h)
        left_rounds = 2 * ng - 2 * HA - 1
        many = HA * NP
        e = (now - 2 * HA - 1) * many
        for h in range(HA, 2 * HA):
            p = lax.div(e, left_rounds) - (h - HA) * NP

            @pl.when((e >= 0) & (lax.rem(e, left_rounds) < many) & (p >= 0) & (p < NP))
            def _():
                ag.arrived(p, h)

    @pl.when(g == ng - 1)
    def _():
        ag.end(NP)


def gather(axis, side, sh, dc, og, ln, dy, gathered, PU=2, NB=256):
    nl, RR, D = sh.shape
    nu = gathered.shape[0]
    CF, T = dc.shape
    dF = og.shape[0]
    NP = nl // PU
    hops = 2 * (side - 1)
    dma = pltpu.SemaphoreType.DMA
    anyspace = pl.BlockSpec(memory_space=pl.ANY)
    return pl.pallas_call(
        functools.partial(gather_kernel, axis, side, nu - nl, PU),
        grid=(D // NB,),
        in_specs=[anyspace] * 3 + [pl.BlockSpec((T, NB), lambda t: (0, t))] * 2 + [anyspace],
        out_specs=[pl.BlockSpec((CF, NB), lambda t: (0, t)), pl.BlockSpec((dF, NB), lambda t: (0, t)), anyspace],
        out_shape=[jax.ShapeDtypeStruct((CF, D), BF), jax.ShapeDtypeStruct((dF, D), BF),
                   jax.ShapeDtypeStruct(gathered.shape, BF)],
        scratch_shapes=[pltpu.VMEM((nl, RR, D), BF), pltpu.VMEM((CF, T), BF), pltpu.VMEM((dF, T), BF),
                        dma, dma((2,)), dma((2,)),
                        dma((NP, COLORS, hops)), dma((NP, COLORS, hops)), dma, dma, dma((NP,))],
        input_output_aliases={5: 2},
        compiler_params=pltpu.CompilerParams(vmem_limit_bytes=VMEM_LIMIT, collective_id=2, has_side_effects=True),
        name="gather_grads",
    )(sh, dc, og, ln, dy, gathered)


def finish_kernel(d, C, o1_ref, o2_ref, gh_ref, gw_ref, gd_ref, gq_ref, gu_ref, dx_ref, buf, isem, osem):
    g = pl.program_id(0)
    ng = pl.num_programs(0)
    R = buf.shape[1]

    def cin(a):
        return pltpu.make_async_copy(gh_ref.at[pl.ds(pl.multiple_of(a * R, R), R), :], buf.at[lax.rem(a, 4)], isem.at[lax.rem(a, 4)])

    def cout(a):
        return pltpu.make_async_copy(buf.at[lax.rem(a, 4)], dx_ref.at[pl.ds(pl.multiple_of(a * R, R), R), :], osem.at[lax.rem(a, 4)])

    @pl.when(g == 0)
    def _():
        cin(0).start()
        cin(1).start()
    for j in range(2):
        a = 2 * g + j
        cin(a).wait()
        cout(a).start()

        @pl.when(g > 0)
        def _():
            cout(a - 2).wait()

        @pl.when(g < ng - 1)
        def _():
            cin(a + 2).start()
    gw_ref[...] = o2_ref[:d, :]
    gd_ref[...] = o2_ref[d:, :]
    gq_ref[...] = o1_ref[:C, :].T
    gu_ref[...] = o1_ref[C:, :].T

    @pl.when(g == ng - 1)
    def _():
        cout(2 * g).wait()
        cout(2 * g + 1).wait()


def finish(d, C, o1, o2, gathered, NB=512):
    T, D = gathered.shape
    CF, dF = o1.shape[0], o2.shape[0]
    steps = D // NB
    R = T // (2 * steps)
    return pl.pallas_call(
        functools.partial(finish_kernel, d, C),
        grid=(steps,),
        in_specs=[pl.BlockSpec((CF, NB), lambda t: (0, t)),
                  pl.BlockSpec((dF, NB), lambda t: (0, t)),
                  pl.BlockSpec(memory_space=pl.ANY)],
        out_specs=[pl.BlockSpec((d, NB), lambda t: (0, t)), pl.BlockSpec((dF - d, NB), lambda t: (0, t)),
                   pl.BlockSpec((NB, C), lambda t: (t, 0)), pl.BlockSpec((NB, CF - C), lambda t: (t, 0)),
                   pl.BlockSpec(memory_space=pl.ANY)],
        out_shape=[jax.ShapeDtypeStruct((d, D), BF), jax.ShapeDtypeStruct((dF - d, D), BF),
                   jax.ShapeDtypeStruct((D, C), BF), jax.ShapeDtypeStruct((D, CF - C), BF),
                   jax.ShapeDtypeStruct((T, D), BF)],
        scratch_shapes=[pltpu.VMEM((4, R, D), BF), pltpu.SemaphoreType.DMA((4,)), pltpu.SemaphoreType.DMA((4,))],
        compiler_params=pltpu.CompilerParams(vmem_limit_bytes=VMEM_LIMIT),
        name="finish_grads",
    )(o1, o2, gathered)


def solution(mesh):
    row_spec = P('dp', None, None)
    in_specs = (row_spec, P(None), P(None), P(None, 'tp', None), P('tp', None), P(None, 'tp'), P('tp', None), row_spec)
    out_specs = (row_spec, P('dp', 'tp', None), P(('dp', 'tp'), None), P('dp', 'tp'), P(('dp', 'tp'), None))
    chips = mesh.shape['tp'] // CORES
    side = int(round(chips ** 0.5))
    assert side * side == chips

    def device_step(tokens, ln_gain, ln_bias, w_qkv, w_out, w_up, w_down, grad_out):
        rows, seq, D = tokens.shape
        T = rows * seq
        C = w_qkv.shape[1] * w_qkv.shape[2]
        d = w_out.shape[0]
        x = tokens.reshape(T, D)
        dy = grad_out.reshape(T, D)
        ln, dc, og, sh, gathered = forward('tp', side, x, dy, ln_gain, ln_bias, w_qkv.reshape(D, C), w_up, w_out, w_down, seq)
        o1, o2, gathered = gather('tp', side, sh, dc, og, ln, dy, gathered)
        gw, gd, gq, gu, dx = finish(d, C, o1, o2, gathered.reshape(T, D))
        return dx.reshape(tokens.shape), gq.reshape(w_qkv.shape), gw, gu, gd

    return jax.shard_map(device_step, mesh=mesh, in_specs=in_specs, out_specs=out_specs, check_vma=False)
```

```python
import functools
import jax
import jax.numpy as jnp
from jax import lax
from jax.experimental import pallas as pl
from jax.experimental.pallas import tpu as pltpu
from jax.sharding import PartitionSpec as P

EPS = 1e-5
GELU_COEF = 0.7071067811865476
PDF_COEF = 0.3989422804014327
F32 = jnp.float32
BF = jnp.bfloat16
VMEM_LIMIT = 64 * 2**20 - 65536
CORES = 2
COLORS = 4
AG_EVERY = 32
NB = 512


def dg(a, b, ca, cb):
    return lax.dot_general(a, b, (((ca,), (cb,)), ((), ())), preferred_element_type=F32)


def normalize(x):
    x = x.astype(F32)
    c = x - jnp.mean(x, axis=-1, keepdims=True)
    r = lax.rsqrt(jnp.mean(c * c, axis=-1, keepdims=True) + EPS)
    return c * r, r


def ln_rows(x_ref, dst, rows, g_ref, b_ref, CH=512):
    D = x_ref.shape[1]
    tot = sq = None
    for c in range(0, D, CH):
        v = jnp.sum(x_ref[rows, c:c + CH].astype(F32), axis=-1, keepdims=True)
        tot = v if tot is None else tot + v
    mean = tot * (1.0 / D)
    for c in range(0, D, CH):
        v = x_ref[rows, c:c + CH].astype(F32) - mean
        v = jnp.sum(v * v, axis=-1, keepdims=True)
        sq = v if sq is None else sq + v
    r = lax.rsqrt(sq * (1.0 / D) + EPS)
    for c in range(0, D, CH):
        v = x_ref[rows, c:c + CH].astype(F32) - mean
        dst[rows, c:c + CH] = (v * r * g_ref[:, c:c + CH] + b_ref[:, c:c + CH]).astype(BF)


class Tile:
    def __init__(self, ln, dy, wt, wd, dct, qkv_s, do_s, h_s, da_s, og_ref, dc_ref, st_s, dp_s, p_b, ds_b, C, F, d, store):
        self.ln, self.dy, self.wt, self.wd, self.dct = ln, dy, wt, wd, dct
        self.qkv_s, self.do_s, self.h_s, self.da_s = qkv_s, do_s, h_s, da_s
        self.og_ref, self.dc_ref, self.st_s, self.dp_s, self.p_b, self.ds_b = og_ref, dc_ref, st_s, dp_s, p_b, ds_b
        self.C, self.F, self.d, self.store = C, F, d, store
        self.S, self.D = ln.shape

    def project(self, side, pieces):
        wt, wd, C, d, half = self.wt, self.wd, self.C, self.d, self.F // 2

        def more(j):
            for i in range(pieces * j // 5, pieces * (j + 1) // 5):
                side(i)
        self.qkv_s[...] = dg(wt[:C, :], self.ln[...], 1, 1).astype(BF)
        more(0)
        y = dg(wd[:d + half, :], self.dy[...], 1, 1)
        self.do_s[...] = y[:d].astype(BF)
        self.da_s[:half, :] = y[d:]
        more(1)
        self.h_s[:half, :] = dg(wt[C:C + half, :], self.ln[...], 1, 1)
        more(2)
        self.da_s[half:, :] = dg(wd[d + half:, :], self.dy[...], 1, 1)
        more(3)
        self.h_s[half:, :] = dg(wt[C + half:, :], self.ln[...], 1, 1)
        more(4)

    def col(self, i):
        self.store(i, dg(self.dct[...], self.wt[:, i * NB:(i + 1) * NB], 1, 0).astype(BF))

    def gelu(self, i, n):
        for j in range(2):
            r0 = (2 * i + j) * n
            h = self.h_s[r0:r0 + n, :]
            cdf = 0.5 * (1.0 + lax.erf(h * GELU_COEF))
            self.og_ref[self.d + r0:self.d + r0 + n, :] = (h * cdf).astype(BF)
            slope = cdf + h * PDF_COEF * jnp.exp(-0.5 * h * h)
            self.dc_ref[self.C + r0:self.C + r0 + n, :] = (self.da_s[r0:r0 + n, :] * slope).astype(BF)

    def softmax(self, scale, QC=128):
        S = self.S
        for c in range(0, S, QC):
            kk = c + QC
            qs = slice(c, c + QC)
            st = self.st_s[:kk, qs] * scale
            ki = lax.broadcasted_iota(jnp.int32, (kk, QC), 0)
            qi = lax.broadcasted_iota(jnp.int32, (kk, QC), 1) + c
            st = jnp.where(ki <= qi, st, -1e30)
            e = jnp.exp(st - jnp.max(st, axis=0, keepdims=True))
            p = e / jnp.sum(e, axis=0, keepdims=True)
            dp = self.dp_s[:kk, qs]
            rd = jnp.sum(p * dp, axis=0, keepdims=True)
            self.p_b[:kk, qs] = p.astype(BF)
            self.ds_b[:kk, qs] = (p * (dp - rd) * scale).astype(BF)
            if kk < S:
                self.p_b[kk:, qs] = jnp.zeros((S - kk, QC), BF)
                self.ds_b[kk:, qs] = jnp.zeros((S - kk, QC), BF)

    def rest(self):
        d = self.d
        scale = d ** -0.5
        n = self.D // NB
        rows = self.F // (2 * n)
        q, k, v, do = self.qkv_s[:d, :], self.qkv_s[d:2 * d, :], self.qkv_s[2 * d:3 * d, :], self.do_s[...]
        self.col(0)
        self.st_s[...] = dg(k, q, 0, 0)
        self.dp_s[...] = dg(v, do, 0, 0)
        self.col(1)
        self.gelu(0, rows)
        self.gelu(1, rows)
        self.softmax(scale)
        self.col(2)
        self.gelu(2, rows)
        self.og_ref[:d, :] = dg(v, self.p_b[...], 1, 0).astype(BF)
        self.dc_ref[2 * d:3 * d, :] = dg(do, self.p_b[...], 1, 1).astype(BF)
        self.col(3)
        self.gelu(3, rows)
        self.dc_ref[:d, :] = dg(k, self.ds_b[...], 1, 0).astype(BF)
        self.dc_ref[d:2 * d, :] = dg(q, self.ds_b[...], 1, 1).astype(BF)
        for i in range(4, n):
            self.col(i)
            self.gelu(i, rows)
        self.dct[...] = self.dc_ref[...].T

    def last(self):
        for i in range(self.D // NB):
            self.col(i)


class Place:
    def __init__(self, axis, side):
        self.axis, self.side = axis, side
        i = lax.axis_index(axis)
        self.c = lax.rem(i, CORES)
        chip = lax.div(i, CORES)
        x, y = lax.rem(chip, side), lax.div(chip, side)
        self.at = {"x": [x] + [lax.rem(x + j, side) for j in range(1, side)],
                   "y": [y] + [lax.rem(y + j, side) for j in range(1, side)]}
        self.x, self.y = x, y
        self.next = {}
        for sg in (1, -1):
            self.next["x", sg] = self.index(self.block("x", sg), y, self.c)
            self.next["y", sg] = self.index(x, self.block("y", sg), self.c)
        self.other = self.index(x, y, 1 - self.c)

    def index(self, x, y, c):
        return (y * self.side + x) * CORES + c

    def step(self, along, by):
        return self.next[along, by]

    def peer(self):
        return self.other

    def block(self, along, by):
        return self.at[along][by % self.side]

    def partners(self):
        return [self.step("x", 1), self.step("x", -1), self.step("y", 1), self.step("y", -1), self.peer()]

    def greet(self):
        sem = pltpu.get_barrier_semaphore()
        who = self.partners()
        for w in who:
            pl.semaphore_signal(sem, inc=1, device_id={self.axis: w}, device_id_type=pl.DeviceIdType.MESH)
        pl.semaphore_wait(sem, len(who))


RINGS = (("x", "y", 1), ("x", "y", -1), ("y", "x", 1), ("y", "x", -1))


class Gather:
    def __init__(self, me, g_ref, own, base, PU, snd, rcv, p_snd, p_rcv, own_sem):
        self.me, self.g, self.own, self.base, self.PU = me, g_ref, own, base, PU
        self.snd, self.rcv, self.p_snd, self.p_rcv, self.own_sem = snd, rcv, p_snd, p_rcv, own_sem
        self.HA = me.side - 1
        self.CW = g_ref.shape[-1] // COLORS

    def send(self, src, dst, ssem, rsem, dev):
        return pltpu.make_async_remote_copy(src_ref=src, dst_ref=dst, send_sem=ssem, recv_sem=rsem,
                                            device_id={self.me.axis: dev}, device_id_type=pl.DeviceIdType.MESH)

    def units(self, p):
        return pl.ds(self.base + p * self.PU, self.PU)

    def region(self, p, k, h, lag):
        me = self.me
        along_b, along_a, sg = RINGS[k]
        cw = pl.ds(k * self.CW, self.CW)
        if h < self.HA:
            b = me.block(along_a, -sg * lag)
            xi, yi = (me.x, b) if along_a == "y" else (b, me.y)
            return self.g.at[self.units(p), me.c, xi, yi, :, cw]
        b = me.block(along_b, -sg * lag)
        if along_b == "x":
            return self.g.at[self.units(p), me.c, b, :, :, cw]
        return self.g.at[self.units(p), me.c, :, b, :, cw]

    def hop(self, p, k, h):
        along_b, along_a, sg = RINGS[k]
        dst = self.region(p, k, h, h if h < self.HA else h - self.HA)
        src = self.own.at[pl.ds(p * self.PU, self.PU), :, pl.ds(k * self.CW, self.CW)] if h == 0 else dst
        return self.send(src, dst, self.snd.at[p, k, h], self.rcv.at[p, k, h],
                         self.me.step(along_a if h < self.HA else along_b, sg))

    def mine(self, p):
        return self.g.at[self.units(p), self.me.c, self.me.x, self.me.y]

    def keep(self, p):
        return pltpu.make_async_copy(self.own.at[pl.ds(p * self.PU, self.PU)], self.mine(p), self.own_sem.at[p])

    def to_peer(self, src, dst):
        return self.send(src, dst, self.p_snd, self.p_rcv, self.me.peer())

    def begin(self, p):
        for k in range(COLORS):
            self.hop(p, k, 0).start()
        self.keep(p).start()
        self.to_peer(self.own.at[pl.ds(p * self.PU, self.PU)], self.mine(p)).start()

    def arrived(self, p, h):
        HA = self.HA
        if h == HA - 1:
            self.keep(p).wait()
        for k in range(COLORS):
            self.hop(p, k, h).wait()
            if h < 2 * HA - 1:
                self.hop(p, k, h + 1).start()
            got = self.region(p, k, h, (h if h < HA else h - HA) + 1)
            self.to_peer(got, got).start()

    def end(self, count):
        every = self.g.at[pl.ds(self.base, count * self.PU), self.me.c]
        self.to_peer(every, every).wait()


def layer_kernel(axis, side, S, TM, C, F, d, PU, early,
                 x_ref, dy_ref, g_ref, b_ref, wqh_ref, wuh_ref, woh_ref, wdh_ref,
                 lnh_ref, dch_ref, ogh_ref, gat_ref, o1h_ref, o2h_ref,
                 q_s, r1_s, r2_s, fx_s, fd_s, fo_s,
                 w_sem, wst_sem, x_sem, dy_sem, ln_sem, dc_sem, og_sem, s0_send, s0_recv, s1_send, s1_recv, s2_send, s2_recv,
                 f_sem, a_send, a_recv, ap_send, ap_recv, ao_sem, l_sem, b_sem, o_sem):
    T, D = x_ref.shape
    n = side
    me = Place(axis, side)
    nt = T // TM
    nu = nt // 2
    CF, dF = C + F, d + F
    CW = D // COLORS
    QB = q_s.shape[0]
    RB = r1_s.shape[0]
    RR = q_s.shape[3]
    first_steps = nt + 3

    def copy_to(src, dst, ssem, rsem, dev):
        return pltpu.make_async_remote_copy(src_ref=src, dst_ref=dst, send_sem=ssem, recv_sem=rsem,
                                            device_id={axis: dev}, device_id_type=pl.DeviceIdType.MESH)

    def cols(k):
        return pl.ds(k * CW, CW)

    def tile_rows(t):
        return pl.ds(pl.multiple_of(t * TM, TM), TM)

    def q_block(u, k, by):
        along = RINGS[k][0]
        q = q_s.at[lax.rem(u, QB)]
        b = me.block(along, by)
        return q.at[b, :, :, cols(k)] if along == "x" else q.at[:, b, :, cols(k)]

    def st1(u, k, s):
        along, _, sg = RINGS[k]
        rs = lax.rem(u, RB)
        src = q_block(u, k, -sg) if s == 0 else r1_s.at[rs, s - 1, k]
        return copy_to(src, r1_s.at[rs, s, k], s1_send.at[rs, s, k], s1_recv.at[rs, s, k], me.step(along, sg))

    def st2(u, k, s):
        _, along, sg = RINGS[k]
        rs = lax.rem(u, RB)
        src = r1_s.at[rs, n - 2, k, me.block(along, -sg)] if s == 0 else r2_s.at[rs, s - 1, k]
        return copy_to(src, r2_s.at[rs, s, k], s2_send.at[rs, s, k], s2_recv.at[rs, s, k], me.step(along, sg))

    def on_st1(u, s):
        for k in range(COLORS):
            st1(u, k, s).wait()
        rs = lax.rem(u, RB)
        for k in range(COLORS):
            sg = RINGS[k][2]
            own = q_block(u, k, -sg * (2 + s))
            r1_s[rs, s, k] = r1_s[rs, s, k] + own[...]
        for k in range(COLORS):
            (st1(u, k, s + 1) if s < n - 2 else st2(u, k, 0)).start()

    def shard_rows(u):
        r = u * 2 * TM + ((me.c * n + me.x) * n + me.y) * RR
        return pl.ds(pl.multiple_of(r, RR), RR)

    def fetch(u):
        return (pltpu.make_async_copy(x_ref.at[shard_rows(u), :], fx_s, f_sem.at[0]),
                pltpu.make_async_copy(dy_ref.at[shard_rows(u), :], fd_s, f_sem.at[1]))

    ag = Gather(me, gat_ref, fo_s, 0, PU, a_send, a_recv, ap_send, ap_recv, ao_sem)

    def on_st2(u, s):
        for k in range(COLORS):
            st2(u, k, s).wait()
        rs = lax.rem(u, RB)
        for k in range(COLORS):
            along, sg = RINGS[k][1], RINGS[k][2]
            own = r1_s.at[rs, n - 2, k, me.block(along, -sg * (2 + s))]
            r2_s[rs, s, k] = r2_s[rs, s, k] + own[...]
            if s < n - 2:
                st2(u, k, s + 1).start()
        if s == n - 3:
            for f in fetch(u):
                f.start()
        if s == n - 2:
            for f in fetch(u):
                f.wait()
            xhat, r = normalize(fx_s[...])
            total = jnp.concatenate([r2_s[rs, s, k] for k in range(COLORS)], axis=-1).astype(F32)
            dh = total * g_ref[...]
            gx = r * (dh - jnp.mean(dh, axis=-1, keepdims=True) - xhat * jnp.mean(dh * xhat, axis=-1, keepdims=True))
            fo_s[u] = (fd_s[...].astype(F32) + gx).astype(BF)

            @pl.when(lax.rem(u, PU) == PU - 1)
            def _():
                ag.begin(lax.div(u, PU))

    rs_at = (4, 10, 16, 22, 26, 30, 34)
    hops = [functools.partial(on_st1, s=s) for s in range(n - 1)] + [functools.partial(on_st2, s=s) for s in range(n - 1)]

    def reduce_round(g, r, on_st0):
        for rho, fn in reversed(list(zip(rs_at, [on_st0] + hops, strict=True))):
            if rho % 4 != r or fn is None:
                continue
            back = 3 + rho // 4
            u = lax.div(g - back, 2)

            @pl.when((g >= back) & (lax.rem(g - back + 2 * nt, 2) == 0) & (u < nu))
            def _():
                fn(u)

    def phase_one(wt_ref, wd_ref, wq_s, wu_s, x_s, dy_s, ln_s, h_s, da_s, qkv_s, do_s, dct_s, dc_o, og_o, st_s, dp_s, p_b, ds_b, p_s):
        WR = wq_s.shape[1]

        def x_in(t):
            return pltpu.make_async_copy(x_ref.at[tile_rows(t), :], x_s.at[lax.rem(t, 2)], x_sem.at[lax.rem(t, 2)])

        def dy_in(t):
            return pltpu.make_async_copy(dy_ref.at[tile_rows(t), :], dy_s.at[lax.rem(t, 2)], dy_sem.at[lax.rem(t, 2)])

        def ln_out(t):
            return pltpu.make_async_copy(ln_s.at[lax.rem(t, 2)], lnh_ref.at[tile_rows(t), :], ln_sem.at[lax.rem(t, 2)])

        def dc_out(t):
            return pltpu.make_async_copy(dc_o.at[lax.rem(t, 2)], dch_ref.at[:, tile_rows(t)], dc_sem.at[lax.rem(t, 2)])

        def og_out(t):
            return pltpu.make_async_copy(og_o.at[lax.rem(t, 2)], ogh_ref.at[:, tile_rows(t)], og_sem.at[lax.rem(t, 2)])

        def w_in(i):
            rows = pl.ds(pl.multiple_of(i * WR, WR), WR)
            j = lax.rem(i, 2)
            return (pltpu.make_async_copy(wqh_ref.at[rows, :], wq_s.at[j], wst_sem.at[j, 0]),
                    pltpu.make_async_copy(wuh_ref.at[rows, :], wu_s.at[j], wst_sem.at[j, 1]))
        whole = (pltpu.make_async_copy(woh_ref, wd_ref.at[pl.ds(0, d), :], w_sem.at[0]),
                 pltpu.make_async_copy(wdh_ref, wd_ref.at[pl.ds(d, F), :], w_sem.at[1]))
        for cp in (x_in(0),) + w_in(0) + w_in(1) + (x_in(1),) + whole + (dy_in(0),):
            cp.start()
        me.greet()
        dct_s[...] = jnp.zeros_like(dct_s)
        x_in(0).wait()

        def lnb(i, _):
            ln_rows(x_s.at[0], ln_s.at[0], pl.ds(pl.multiple_of(i * 16, 16), 16), g_ref, b_ref)
            return 0
        lax.fori_loop(0, TM // 16, lnb, 0)

        def wtb(i, _):
            for cp in w_in(i):
                cp.wait()
            to = pl.ds(pl.multiple_of(i * WR, WR), WR)
            j = lax.rem(i, 2)
            wt_ref[:C, to] = wq_s[j].T
            wt_ref[C:, to] = wu_s[j].T

            @pl.when(i + 2 < D // WR)
            def _():
                for cp in w_in(i + 2):
                    cp.start()
            return 0
        lax.fori_loop(0, D // WR, wtb, 0)
        for cp in whole:
            cp.wait()

        def st0(u):
            qi = lax.rem(u, QB)
            return copy_to(p_s.at[lax.rem(u, 2), 1 - me.c], q_s.at[qi], s0_send.at[qi], s0_recv.at[qi], me.peer())

        def on_st0(u):
            st0(u).wait()
            qi, pi = lax.rem(u, QB), lax.rem(u, 2)
            for a in range(n):
                for b in range(n):
                    q_s[qi, a, b] = q_s[qi, a, b] + p_s[pi, me.c, a, b]
            for k in range(COLORS):
                st1(u, k, 0).start()

        ag_at = (6, 10, 14, 22, 30, 38)

        def comm(g, r):
            reduce_round(g, r, on_st0)
            now = 4 * g + r
            for h, o in enumerate(ag_at):
                first = 8 * (PU - 1) + 12 + rs_at[-1] + o
                if first % 4 != r:
                    continue
                p = lax.div(now - first, AG_EVERY)

                @pl.when((now >= first) & (lax.rem(now - first + 64 * AG_EVERY, AG_EVERY) == 0) & (p < early))
                def _():
                    ag.arrived(p, h)

        def step(g, _):
            slot = lax.rem(g, 2)
            nxt = 1 - slot
            live = g < nt
            before = g + 3

            def store(i, v):
                p_s[lax.rem(lax.div(before, 2), 2), lax.rem(before, 2), :, :, :, pl.ds(i * NB, NB)] = v.reshape(n, n, RR, NB)
            tile = Tile(ln_s.at[slot], dy_s.at[slot], wt_ref, wd_ref, dct_s, qkv_s, do_s, h_s, da_s,
                        og_o.at[slot], dc_o.at[slot], st_s, dp_s, p_b, ds_b, C, F, d, store)

            @pl.when((g > 0) & (g <= nt))
            def _():
                ln_out(g - 1).wait()

            @pl.when((g > 1) & (g <= nt + 1))
            def _():
                dc_out(g - 2).wait()
                og_out(g - 2).wait()

            @pl.when(g + 2 < nt)
            def _():
                x_in(g + 2).start()

            @pl.when(g + 1 < nt)
            def _():
                dy_in(g + 1).start()
                x_in(g + 1).wait()

            @pl.when(live)
            def _():
                dy_in(g).wait()
                ln_out(g).start()

            comm(g, 0)

            @pl.when(live)
            def _():
                tile.project(lambda i: ln_rows(x_s.at[nxt], ln_s.at[nxt], pl.ds(i * 8, 8), g_ref, b_ref), TM // 8)

            comm(g, 2)

            @pl.when(live)
            def _():
                tile.rest()
                dc_out(g).start()
                og_out(g).start()

            @pl.when(g == nt)
            def _():
                tile.last()

            @pl.when((g > 0) & (g <= nt) & (slot == 0))
            def _():
                st0(lax.div(g, 2) - 1).start()
            return 0
        lax.fori_loop(0, first_steps, step, 0)

    vm = pltpu.VMEM
    WR = 512
    pl.run_scoped(phase_one, vm((CF, D), BF), vm((dF, D), BF), vm((2, WR, C), BF), vm((2, WR, F), BF),
                  vm((2, TM, D), BF), vm((2, TM, D), BF), vm((2, TM, D), BF), vm((F, TM), F32), vm((F, TM), F32),
                  vm((C, TM), BF), vm((d, TM), BF), vm((TM, CF), BF), vm((2, CF, TM), BF), vm((2, dF, TM), BF),
                  vm((S, S), F32), vm((S, S), F32), vm((S, S), BF), vm((S, S), BF),
                  vm((2, CORES, side, side, RR, D), BF))

    NC = 256
    ng = D // NC
    NP = nu // PU
    gap = 5
    at = (0, 1, 2, 5, 8, 11)
    tail = max(0, -(-(gap * (NP - early - 1) + at[-1] + 1 - 2 * ng) // 2))

    def phase_two(dc_s, og_s, lnb_s, dyb_s, o1_s, o2_s):
        def block(i, which):
            cs = pl.ds(pl.multiple_of(i * NC, NC), NC)
            src, dst = ((lnh_ref, lnb_s), (dy_ref, dyb_s))[which]
            return pltpu.make_async_copy(src.at[:, cs], dst, b_sem.at[which])

        def out(i, which):
            cs = pl.ds(pl.multiple_of(i * NC, NC), NC)
            src, dst = ((o1_s, o1h_ref), (o2_s, o2h_ref))[which]
            return pltpu.make_async_copy(src.at[lax.rem(i, 2)], dst.at[:, cs], o_sem.at[which, lax.rem(i, 2)])
        left = (pltpu.make_async_copy(dch_ref, dc_s, l_sem.at[0]), pltpu.make_async_copy(ogh_ref, og_s, l_sem.at[1]))
        left[0].start()
        block(0, 0).start()
        block(0, 1).start()
        left[1].start()

        def comm(g2, r):
            reduce_round(g2 + first_steps, r, None)
            half = 2 * g2 + r // 2
            for h, o in enumerate(at):
                p = lax.div(half - o, gap) + early

                @pl.when((half >= o) & (lax.rem(half - o + 64 * gap, gap) == 0) & (p < NP))
                def _():
                    ag.arrived(p, h)

        def step(g2, _):
            live = g2 < ng
            buf = lax.rem(g2, 2)

            @pl.when(g2 == 0)
            def _():
                left[0].wait()

            for j in range(2):
                src, rhs, o_s, M = ((dc_s, lnb_s, o1_s, CF // 2), (og_s, dyb_s, o2_s, dF // 2))[j]
                comm(g2, 2 * j)

                @pl.when((g2 == 0) & (j == 1))
                def _():
                    left[1].wait()

                @pl.when((g2 > 1) & live)
                def _():
                    out(g2 - 2, j).wait()

                @pl.when(live)
                def _():
                    block(g2, j).wait()
                    for i in range(2):
                        rows = pl.ds(i * M, M)
                        o_s[buf, rows, :] = jnp.dot(src[rows, :], rhs[...], preferred_element_type=F32).astype(BF)
                    out(g2, j).start()

                @pl.when(g2 + 1 < ng)
                def _():
                    block(g2 + 1, j).start()
            return 0
        lax.fori_loop(0, ng + tail, step, 0)
        for j in range(2):
            out(ng - 2, j).wait()
            out(ng - 1, j).wait()
        ag.end(NP)

    pl.run_scoped(phase_two, vm((CF, T), BF), vm((dF, T), BF), vm((T, NC), BF), vm((T, NC), BF),
                  vm((2, CF, NC), BF), vm((2, dF, NC), BF))


def layer(axis, side, x, dy, gain, bias, w_qkv, w_up, w_out, w_down, S, TM=256, PU=2, early=2):
    T, D = x.shape
    C, F, d = w_qkv.shape[1], w_up.shape[1], w_out.shape[0]
    CF, dF = C + F, d + F
    nu = T // TM // 2
    RR = 2 * TM // (CORES * side * side)
    CW = D // COLORS
    QB, RB = 4, 5
    NP = nu // PU
    hops = 2 * (side - 1)
    dma = pltpu.SemaphoreType.DMA
    anyspace = pl.BlockSpec(memory_space=pl.ANY)
    vm = pl.BlockSpec(memory_space=pltpu.VMEM)
    return pl.pallas_call(
        functools.partial(layer_kernel, axis, side, S, TM, C, F, d, PU, early),
        in_specs=[anyspace, anyspace, vm, vm] + [anyspace] * 4,
        out_specs=[anyspace] * 6,
        out_shape=[jax.ShapeDtypeStruct((T, D), BF), jax.ShapeDtypeStruct((CF, T), BF), jax.ShapeDtypeStruct((dF, T), BF),
                   jax.ShapeDtypeStruct((nu, CORES, side, side, RR, D), BF),
                   jax.ShapeDtypeStruct((CF, D), BF), jax.ShapeDtypeStruct((dF, D), BF)],
        scratch_shapes=[pltpu.VMEM((QB, side, side, RR, D), BF),
                        pltpu.VMEM((RB, side - 1, COLORS, side, RR, CW), BF),
                        pltpu.VMEM((RB, side - 1, COLORS, RR, CW), BF),
                        pltpu.VMEM((RR, D), BF), pltpu.VMEM((RR, D), BF), pltpu.VMEM((nu, RR, D), BF),
                        dma((2,)), dma((2, 2)), dma((2,)), dma((2,)), dma((2,)), dma((2,)), dma((2,)), dma((QB,)), dma((QB,)),
                        dma((RB, side - 1, COLORS)), dma((RB, side - 1, COLORS)),
                        dma((RB, side - 1, COLORS)), dma((RB, side - 1, COLORS)),
                        dma((2,)), dma((NP, COLORS, hops)), dma((NP, COLORS, hops)), dma, dma, dma((NP,)),
                        dma((2,)), dma((2,)), dma((2, 2))],
        compiler_params=pltpu.CompilerParams(vmem_limit_bytes=VMEM_LIMIT, collective_id=1, has_side_effects=True),
        name="layer_grads",
    )(x, dy, gain.reshape(1, D), bias.reshape(1, D), w_qkv, w_up, w_out, w_down)


def finish_kernel(d, C, o1_ref, o2_ref, gh_ref, gw_ref, gd_ref, gq_ref, gu_ref, dx_ref, buf, isem, osem):
    g = pl.program_id(0)
    ng = pl.num_programs(0)
    R = buf.shape[1]

    def cin(a):
        return pltpu.make_async_copy(gh_ref.at[pl.ds(pl.multiple_of(a * R, R), R), :], buf.at[lax.rem(a, 4)], isem.at[lax.rem(a, 4)])

    def cout(a):
        return pltpu.make_async_copy(buf.at[lax.rem(a, 4)], dx_ref.at[pl.ds(pl.multiple_of(a * R, R), R), :], osem.at[lax.rem(a, 4)])

    @pl.when(g == 0)
    def _():
        cin(0).start()
        cin(1).start()
    for j in range(2):
        a = 2 * g + j
        cin(a).wait()
        cout(a).start()

        @pl.when(g > 0)
        def _():
            cout(a - 2).wait()

        @pl.when(g < ng - 1)
        def _():
            cin(a + 2).start()
    gw_ref[...] = o2_ref[:d, :]
    gd_ref[...] = o2_ref[d:, :]
    gq_ref[...] = o1_ref[:C, :].T
    gu_ref[...] = o1_ref[C:, :].T

    @pl.when(g == ng - 1)
    def _():
        cout(2 * g).wait()
        cout(2 * g + 1).wait()


def finish(d, C, o1, o2, gathered, NB=512):
    T, D = gathered.shape
    CF, dF = o1.shape[0], o2.shape[0]
    steps = D // NB
    R = T // (2 * steps)
    return pl.pallas_call(
        functools.partial(finish_kernel, d, C),
        grid=(steps,),
        in_specs=[pl.BlockSpec((CF, NB), lambda t: (0, t)),
                  pl.BlockSpec((dF, NB), lambda t: (0, t)),
                  pl.BlockSpec(memory_space=pl.ANY)],
        out_specs=[pl.BlockSpec((d, NB), lambda t: (0, t)), pl.BlockSpec((dF - d, NB), lambda t: (0, t)),
                   pl.BlockSpec((NB, C), lambda t: (t, 0)), pl.BlockSpec((NB, CF - C), lambda t: (t, 0)),
                   pl.BlockSpec(memory_space=pl.ANY)],
        out_shape=[jax.ShapeDtypeStruct((d, D), BF), jax.ShapeDtypeStruct((dF - d, D), BF),
                   jax.ShapeDtypeStruct((D, C), BF), jax.ShapeDtypeStruct((D, CF - C), BF),
                   jax.ShapeDtypeStruct((T, D), BF)],
        scratch_shapes=[pltpu.VMEM((4, R, D), BF), pltpu.SemaphoreType.DMA((4,)), pltpu.SemaphoreType.DMA((4,))],
        compiler_params=pltpu.CompilerParams(vmem_limit_bytes=VMEM_LIMIT),
        name="finish_grads",
    )(o1, o2, gathered)


def solution(mesh):
    row_spec = P('dp', None, None)
    in_specs = (row_spec, P(None), P(None), P(None, 'tp', None), P('tp', None), P(None, 'tp'), P('tp', None), row_spec)
    out_specs = (row_spec, P('dp', 'tp', None), P(('dp', 'tp'), None), P('dp', 'tp'), P(('dp', 'tp'), None))
    chips = mesh.shape['tp'] // CORES
    side = int(round(chips ** 0.5))
    assert side * side == chips

    def device_step(tokens, ln_gain, ln_bias, w_qkv, w_out, w_up, w_down, grad_out):
        rows, seq, D = tokens.shape
        T = rows * seq
        C = w_qkv.shape[1] * w_qkv.shape[2]
        d = w_out.shape[0]
        x = tokens.reshape(T, D)
        dy = grad_out.reshape(T, D)
        _, _, _, gathered, o1, o2 = layer('tp', side, x, dy, ln_gain, ln_bias, w_qkv.reshape(D, C), w_up, w_out, w_down, seq)
        gw, gd, gq, gu, dx = finish(d, C, o1, o2, gathered.reshape(T, D))
        return dx.reshape(tokens.shape), gq.reshape(w_qkv.shape), gw, gu, gd

    return jax.shard_map(device_step, mesh=mesh, in_specs=in_specs, out_specs=out_specs, check_vma=False)
```
